64 devices in a mesh: replica: 4 (over x, y), pool: 16 (over z, core).
Axes of the slice: x: 2, y: 2, z: 8, core: 2. Of those that a mesh axis runs over, the one named last changes fastest.
The devices are a block of a 4x4x8 slice.
Arguments:
- pool: bfloat16 [2, 2048, 2, 256, 2, 128], P(None, ('replica', 'pool')), parts along dimension 1
- page_idx: int32 [16, 64, 4], P(None, ('replica', 'pool')), parts along dimension 1
- count: int32 [64, 16], P(('replica', 'pool')), parts along dimension 0
- x: bfloat16 [64, 64, 2048], P(('replica', 'pool')), parts along dimension 0
- norm_attn: bfloat16 [2, 2048], replicated
- wq: bfloat16 [2, 2048, 2048], replicated
- wk: bfloat16 [2, 2048, 256], replicated
- wv: bfloat16 [2, 2048, 256], replicated
- wo: bfloat16 [2, 2048, 2048], replicated
- norm_mlp: bfloat16 [2, 2048], replicated
- w_gate: bfloat16 [2, 2048, 11008], replicated
- w_up: bfloat16 [2, 2048, 11008], replicated
- w_down: bfloat16 [2, 11008, 2048], replicated
Outputs:
- output: bfloat16 [64, 64, 2048], P(('replica', 'pool')), parts along dimension 0
There are 4 independent parts. The reference program is written for one: setup_inputs(seed, part) draws one part's arguments, and reference() takes and returns one part's arrays. A program takes and returns all parts, laid end to end along the dimension named above; an argument that names none is the same for every part.
All inputs are finite; a program needn't handle non-finite values.
Results may differ from the reference program's by a relative error of at most 0.0156482.
Values are sent between devices in bfloat16 or wider.
A program may use at most 768 MiB of HBM per device.

```python
import jax
import jax.numpy as jnp
from jax import lax

GROUP = 16
LAYERS = 2
TOKENS = 64
SLOTS = 4
PAGES = 32
PAGE = 256
D_MODEL = 2048
HEADS = 16
KV_HEADS = 2
HEAD = 128
FF_WIDTH = 11008
HOT_OWNERS = 2
EPS = 1e-5
ROPE_BASE = 500000.0


def draw_normal(one_key, shape, scale):
    return (jax.random.normal(one_key, shape, jnp.float32) * scale).astype(jnp.bfloat16)


def setup_inputs(seed: int = 0, part: int = 0) -> dict:
    part_key = jax.random.fold_in(jax.random.key(seed), part)
    pool_key, page_key, hot_key, small_key, token_key = jax.random.split(part_key, 5)
    shared = jax.random.split(jax.random.key(seed + 1), 9)
    pool = draw_normal(pool_key, (LAYERS, GROUP * PAGES, 2, PAGE, KV_HEADS, HEAD), 1.0)
    pair_keys = jax.random.split(page_key, GROUP * GROUP)
    picks = jax.vmap(lambda one_key: jax.random.permutation(one_key, PAGES)[:SLOTS])(pair_keys)
    page_idx = picks.reshape(GROUP, GROUP, SLOTS).astype(jnp.int32)
    owner_rank = jax.random.permutation(hot_key, GROUP)
    small_counts = jax.random.randint(small_key, (GROUP, GROUP), 0, SLOTS // 4 + 1)
    count = jnp.where(owner_rank[None, :] < HOT_OWNERS, SLOTS, small_counts).astype(jnp.int32)
    x = draw_normal(token_key, (GROUP, TOKENS, D_MODEL), 1.0)
    attn_width = HEADS * HEAD
    kv_width = KV_HEADS * HEAD
    out_gain = ((GROUP * SLOTS * PAGE // 4 + TOKENS) / 4.0) ** 0.5
    return {
        'pool': pool,
        'page_idx': page_idx,
        'count': count,
        'x': x,
        'norm_attn': (1.0 + 0.2 * jax.random.normal(shared[0], (LAYERS, D_MODEL), jnp.float32)).astype(jnp.bfloat16),
        'wq': draw_normal(shared[1], (LAYERS, D_MODEL, attn_width), D_MODEL ** -0.5),
        'wk': draw_normal(shared[2], (LAYERS, D_MODEL, kv_width), D_MODEL ** -0.5),
        'wv': draw_normal(shared[3], (LAYERS, D_MODEL, kv_width), D_MODEL ** -0.5),
        'wo': draw_normal(shared[4], (LAYERS, attn_width, D_MODEL), out_gain * attn_width ** -0.5),
        'norm_mlp': (1.0 + 0.2 * jax.random.normal(shared[5], (LAYERS, D_MODEL), jnp.float32)).astype(jnp.bfloat16),
        'w_gate': draw_normal(shared[6], (LAYERS, D_MODEL, FF_WIDTH), D_MODEL ** -0.5),
        'w_up': draw_normal(shared[7], (LAYERS, D_MODEL, FF_WIDTH), D_MODEL ** -0.5),
        'w_down': draw_normal(shared[8], (LAYERS, FF_WIDTH, D_MODEL), FF_WIDTH ** -0.5),
    }


def rms_norm(vals, gain):
    vals_f = vals.astype(jnp.float32)
    inv_rms = lax.rsqrt(jnp.mean(vals_f * vals_f, axis=-1, keepdims=True) + EPS)
    return (vals_f * inv_rms * gain.astype(jnp.float32)).astype(jnp.bfloat16)


def rotate(proj, tokens):
    half = proj.shape[-1] // 2
    freqs = ROPE_BASE ** (-jnp.arange(half, dtype=jnp.float32) / half)
    angles = jnp.arange(tokens, dtype=jnp.float32)[:, None] * freqs[None, :]
    cos_t = jnp.cos(angles)[:, None, :]
    sin_t = jnp.sin(angles)[:, None, :]
    first = proj[..., :half]
    second = proj[..., half:]
    return jnp.concatenate([first * cos_t - second * sin_t, second * cos_t + first * sin_t], axis=-1)


def request_layer(x_req, layer_args, count_row, page_rows):
    layer_pool, g_attn, wq_l, wk_l, wv_l, wo_l, g_mlp, wg_l, wu_l, wd_l = layer_args
    tokens = x_req.shape[0]
    q_per_kv = HEADS // KV_HEADS
    prefix_len = GROUP * SLOTS * PAGE
    h_attn = rms_norm(x_req, g_attn)
    q_proj = jnp.dot(h_attn, wq_l, preferred_element_type=jnp.float32).reshape(tokens, HEADS, HEAD)
    k_proj = jnp.dot(h_attn, wk_l, preferred_element_type=jnp.float32).reshape(tokens, KV_HEADS, HEAD)
    q_rot = rotate(q_proj, tokens).astype(jnp.bfloat16)
    k_new = rotate(k_proj, tokens).astype(jnp.bfloat16)
    v_new = jnp.dot(h_attn, wv_l, preferred_element_type=jnp.float32).astype(jnp.bfloat16).reshape(tokens, KV_HEADS, HEAD)
    pages = layer_pool.reshape(GROUP, PAGES, 2, PAGE, KV_HEADS, HEAD)
    fetched = pages[jnp.arange(GROUP)[:, None], page_rows]
    k_all = jnp.concatenate([fetched[:, :, 0].reshape(prefix_len, KV_HEADS, HEAD), k_new], axis=0)
    v_all = jnp.concatenate([fetched[:, :, 1].reshape(prefix_len, KV_HEADS, HEAD), v_new], axis=0)
    slot_ok = jnp.arange(SLOTS)[None, :] < count_row[:, None]
    pre_ok = jnp.broadcast_to(slot_ok[:, :, None], (GROUP, SLOTS, PAGE)).reshape(prefix_len)
    causal = jnp.arange(tokens)[None, :] <= jnp.arange(tokens)[:, None]
    allowed = jnp.concatenate([jnp.broadcast_to(pre_ok[None, :], (tokens, prefix_len)), causal], axis=1)
    q_group = q_rot.reshape(tokens, KV_HEADS, q_per_kv, HEAD)
    scores = jnp.einsum('tgrd,kgd->grtk', q_group.astype(jnp.float32), k_all.astype(jnp.float32)) * (HEAD ** -0.5)
    scores = jnp.where(allowed[None, None], scores, -1e30)
    probs = jax.nn.softmax(scores, axis=-1).astype(jnp.bfloat16)
    attn = jnp.einsum('grtk,kgd->tgrd', probs.astype(jnp.float32), v_all.astype(jnp.float32)).astype(jnp.bfloat16).reshape(tokens, HEADS * HEAD)
    x_mid = (x_req.astype(jnp.float32) + jnp.dot(attn, wo_l, preferred_element_type=jnp.float32)).astype(jnp.bfloat16)
    h_mlp = rms_norm(x_mid, g_mlp)
    gate = jnp.dot(h_mlp, wg_l, preferred_element_type=jnp.float32)
    up_proj = jnp.dot(h_mlp, wu_l, preferred_element_type=jnp.float32)
    gated = (jax.nn.silu(gate) * up_proj).astype(jnp.bfloat16)
    return (x_mid.astype(jnp.float32) + jnp.dot(gated, wd_l, preferred_element_type=jnp.float32)).astype(jnp.bfloat16)


def reference(pool, page_idx, count, x, norm_attn, wq, wk, wv, wo, norm_mlp, w_gate, w_up, w_down):
    layer_stack = (pool, norm_attn, wq, wk, wv, wo, norm_mlp, w_gate, w_up, w_down)

    def one_request(req_args):
        x_req, count_row, page_rows = req_args

        def body(carry, layer_args):
            return request_layer(carry, layer_args, count_row, page_rows), None

        result, unused = lax.scan(body, x_req, layer_stack)
        return result

    return lax.map(one_request, (x, count, page_idx))
```

```python
import functools

import jax
import jax.numpy as jnp
from jax import lax
from jax.experimental import pallas as pl
from jax.experimental.pallas import tpu as pltpu
from jax.sharding import PartitionSpec as P

EPS = 1e-5
ROPE_BASE = 500000.0
NEG = -1e30
LOG2E = 1.4426950408889634
CHUNK = 512
DOWN = 256
PAIRS = 3
DOWNS = 3


def rms_norm(vals_f, gain):
    inv_rms = lax.rsqrt(jnp.mean(vals_f * vals_f, axis=-1, keepdims=True) + EPS)
    return (vals_f * inv_rms * gain).astype(jnp.bfloat16)


def dot32(a, b):
    return jnp.dot(a, b, preferred_element_type=jnp.float32)


def kernel(dims, tab, x_ref, cos_ref, sin_ref, ga_ref, gm_ref, kp, vp, wq, wk, wv, wo, wg, wu, wd, out_ref,
           xs, hs, avec, us, qbuf, acc, kpg, vpg, knew, vnew, scores, sent, got, wqo, wkv, gu, dn,
           q_ss, q_rs, a_ss, a_rs, pg_ls, pg_ss, pg_rs, x_ss, x_rs, p_ss, p_rs, wq_s, wkv_s, gu_s, dn_s):
    group, slots = dims
    chips = group // 2
    layers, _, d_model = ga_ref.shape
    tokens = x_ref.shape[0]
    hd = kp.shape[-1]
    page = kp.shape[3]
    pages = kp.shape[2]
    width = wq.shape[2] // 2
    heads = width // hd
    part = tokens // 2
    rows = heads * part
    ff = wg.shape[2] // 2
    n_gu = -(-ff // CHUNK)
    n_dn = d_model // DOWN
    n_out = d_model // CHUNK
    scale = hd ** -0.5 * LOG2E

    me = lax.axis_index("pool")
    z = me // 2
    c = me % 2
    mate = me + 1 - 2 * c

    def along(b):
        delta = jnp.where(b < 2, 1, chips - 1)
        return lax.rem(z + delta, chips) * 2 + c

    def to(dev):
        return {"pool": dev}

    def q_hop(layer, s, b):
        return pltpu.make_async_remote_copy(
            src_ref=qbuf.at[layer, s, b], dst_ref=qbuf.at[layer, s + 1, b], send_sem=q_ss.at[layer, s, b], recv_sem=q_rs.at[layer, s + 1, b],
            device_id=to(along(b)), device_id_type=pl.DeviceIdType.MESH)

    def a_hop(layer, s, b):
        return pltpu.make_async_remote_copy(
            src_ref=acc.at[layer, s, b], dst_ref=acc.at[layer, s + 1, b], send_sem=a_ss.at[layer, s, b], recv_sem=a_rs.at[layer, s + 1, b],
            device_id=to(along(b)), device_id_type=pl.DeviceIdType.MESH)

    def page_local(layer, which):
        src, dst = (kp, kpg) if which == 0 else (vp, vpg)
        return pltpu.make_async_copy(src.at[layer, c], dst.at[c], pg_ls.at[layer, which])

    def page_remote(layer, which):
        src, dst = (kp, kpg) if which == 0 else (vp, vpg)
        return pltpu.make_async_remote_copy(
            src_ref=src.at[layer, 1 - c], dst_ref=dst.at[c], send_sem=pg_ss.at[layer, which], recv_sem=pg_rs.at[layer, which],
            device_id=to(mate), device_id_type=pl.DeviceIdType.MESH)

    def part_hop(layer, k, n, size):
        cols = pl.ds(pl.multiple_of(n * size, size), size)
        return pltpu.make_async_remote_copy(
            src_ref=sent.at[k, :, cols], dst_ref=got.at[k, :, cols], send_sem=p_ss.at[layer, k, n], recv_sem=p_rs.at[layer, k, n],
            device_id=to(mate), device_id_type=pl.DeviceIdType.MESH)

    def load_wq(layer):
        cols = pl.ds(pl.multiple_of(c * width, width), width)
        return [pltpu.make_async_copy(wq.at[layer, :, cols], wqo, wq_s.at[0])]

    def load_wkv(layer):
        cols = pl.ds(pl.multiple_of(c * hd, hd), hd)
        return [pltpu.make_async_copy(w.at[layer, :, cols], wkv.at[i], wkv_s.at[i]) for i, w in enumerate((wk, wv))]

    def load_wo(layer):
        line = pl.ds(pl.multiple_of(c * width, width), width)
        return [pltpu.make_async_copy(wo.at[layer, line, pl.ds(i * width, width)], wqo.at[pl.ds(i * width, width), :], wq_s.at[1 + i])
                for i in range(2)]

    def gu_start(i):
        return pl.multiple_of(jnp.minimum(i * CHUNK, ff - CHUNK), 128)

    def load_gu(layer, i, slot):
        cols = pl.ds(pl.multiple_of(c * ff + gu_start(i), 128), CHUNK)
        return [pltpu.make_async_copy(w.at[layer, :, cols], gu.at[slot, j], gu_s.at[slot, j]) for j, w in enumerate((wg, wu))]

    def load_dn(layer, i, slot):
        line = pl.ds(pl.multiple_of(c * ff, 128), ff)
        return [pltpu.make_async_copy(wd.at[layer, line, pl.ds(pl.multiple_of(i * DOWN, DOWN), DOWN)], dn.at[slot], dn_s.at[slot])]

    def go(copies):
        for one in copies:
            one.start()

    def done(copies):
        for one in copies:
            one.wait()

    barrier = pltpu.get_barrier_semaphore()
    for dev in (mate, along(0), along(2)):
        pl.semaphore_signal(barrier, inc=1, device_id=to(dev), device_id_type=pl.DeviceIdType.MESH)
    go(load_wq(0) + load_wkv(0))
    go([page_local(0, 0), page_local(0, 1)])
    pl.semaphore_wait(barrier, 3)

    own = pl.ds(pl.multiple_of(c * tokens, tokens), tokens)
    x_swap = pltpu.make_async_remote_copy(
        src_ref=x_ref, dst_ref=xs.at[own], send_sem=x_ss, recv_sem=x_rs, device_id=to(mate), device_id_type=pl.DeviceIdType.MESH)
    x_swap.start()
    go([page_remote(0, 0), page_remote(0, 1)])
    xs[own, :] = x_ref[...]
    for i in range(PAIRS):
        go(load_gu(0, i, i))
    for i in range(DOWNS):
        go(load_dn(0, i, i))
    x_swap.wait()

    def attend(q_t, req, extra):
        spots = [(o, j) for o in range(2) for j in range(slots)]
        valid, peaks = [], []
        for n, (o, j) in enumerate(spots):
            owner = 2 * z + o
            s = dot32(kpg[o, tab[owner, req * slots + j]], q_t)
            scores[n] = s
            ok = j < tab[req, group * slots + owner]
            valid.append(ok)
            peaks.append(jnp.where(ok, jnp.max(s, axis=0, keepdims=True) * scale, NEG))
        top = functools.reduce(jnp.maximum, peaks)
        if extra is not None:
            new_s = extra[0]
            top = jnp.maximum(top, jnp.max(new_s, axis=0, keepdims=True) * scale)
        total = jnp.zeros_like(top)
        out = jnp.zeros((hd, rows), jnp.float32)
        for n, (o, j) in enumerate(spots):
            owner = 2 * z + o
            shift = jnp.where(valid[n], -top, NEG)
            p = jnp.exp2(scores[n] * scale + shift)
            total = total + jnp.sum(p, axis=0, keepdims=True)
            out = out + dot32(vpg[o, tab[owner, req * slots + j]], p.astype(jnp.bfloat16))
        if extra is not None:
            p = jnp.exp2(new_s * scale - top)
            total = total + jnp.sum(p, axis=0, keepdims=True)
            out = out + dot32(extra[1], p.astype(jnp.bfloat16))
        return out, top, total

    def put_acc(layer, s, b, out, top, total):
        acc[layer, s, b, :hd, :] = out
        line = lax.broadcasted_iota(jnp.int32, (8, rows), 0)
        acc[layer, s, b, hd:hd + 8, :] = jnp.where(line == 0, top, total)

    def merge(layer, s, b, out, top, total):
        in_out, in_top, in_total = acc[layer, s, b, :hd, :], acc[layer, s, b, hd:hd + 1, :], acc[layer, s, b, hd + 1:hd + 2, :]
        best = jnp.maximum(top, in_top)
        fa, fb = jnp.exp2(in_top - best), jnp.exp2(top - best)
        return in_out * fa + out * fb, best, in_total * fa + total * fb

    def rope(vals):
        return vals * cos_ref[...] + pltpu.roll(vals, hd // 2, axis=1) * sin_ref[...]

    def layer_body(layer, carry):
        last = layer == layers - 1
        hs[...] = rms_norm(xs[...].astype(jnp.float32), ga_ref[layer])
        done(load_wkv(layer))
        k_all = rope(dot32(hs[...], wkv[0])).astype(jnp.bfloat16)
        v_all = dot32(hs[...], wkv[1])
        for i in range(2):
            knew[i] = k_all[i * tokens:(i + 1) * tokens]
            vnew[i] = v_all[i * tokens:(i + 1) * tokens].T.astype(jnp.bfloat16)
        done(load_wq(layer))
        for n in range(heads):
            q_head = rope(dot32(hs[...], wqo[:, n * hd:(n + 1) * hd])).astype(jnp.bfloat16)
            avec[:, n * hd:(n + 1) * hd] = q_head
        for b in range(4):
            lo = (b % 2) * tokens + (b // 2) * part
            q_rows = jnp.concatenate([avec[lo:lo + part, n * hd:(n + 1) * hd] for n in range(heads)], axis=0)
            qbuf[layer, 0, b] = q_rows.astype(jnp.float32).T.astype(jnp.bfloat16)
            q_hop(layer, 0, b).start()
        go(load_wo(layer))

        @pl.when(layer + 1 < layers)
        def _():
            go(load_wkv(layer + 1))

        for b in range(4):
            put_acc(layer, 1, b, jnp.zeros((hd, rows), jnp.float32), jnp.full((1, rows), NEG), jnp.zeros((1, rows), jnp.float32))
        for which in range(2):
            page_local(layer, which).wait()
            page_remote(layer, which).wait()

        def home(b, carry):
            i = lax.rem(b, 2)
            q_t = qbuf[layer, 0, b]
            s = dot32(knew[i], q_t)
            key = lax.broadcasted_iota(jnp.int32, s.shape, 0)
            tok = lax.rem(lax.broadcasted_iota(jnp.int32, s.shape, 1), part) + (b // 2) * part
            s = jnp.where(key <= tok, s, NEG)
            put_acc(layer, 0, b, *attend(q_t, 2 * z + i, (s, vnew[i])))
            return carry

        lax.fori_loop(0, 4, home, 0)

        def step(s, carry):
            for b in range(4):
                q_hop(layer, s - 1, b).wait_recv()

                @pl.when(s < chips - 1)
                def _():
                    q_hop(layer, s, b).start()

            def block(b, carry):
                source = lax.rem(z + jnp.where(b < 2, chips - s, s), chips)
                found = attend(qbuf[layer, s, b], 2 * source + lax.rem(b, 2), None)

                @pl.when(s >= 2)
                def _():
                    a_hop(layer, s - 1, b).wait_recv()

                put_acc(layer, s, b, *merge(layer, s, b, *found))
                a_hop(layer, s, b).start()
                return carry

            return lax.fori_loop(0, 4, block, carry)

        lax.fori_loop(1, chips, step, 0)

        for b in range(4):
            a_hop(layer, chips - 1, b).wait_recv()
            out, top, total = merge(layer, chips, b, acc[layer, 0, b, :hd, :], acc[layer, 0, b, hd:hd + 1, :], acc[layer, 0, b, hd + 1:hd + 2, :])
            a_rows = (out / total).T.astype(jnp.bfloat16)
            lo = (b % 2) * tokens + (b // 2) * part
            for n in range(heads):
                avec[lo:lo + part, n * hd:(n + 1) * hd] = a_rows[n * part:(n + 1) * part]

        def drain(s, carry):
            for b in range(4):
                q_hop(layer, s, b).wait_send()
                a_hop(layer, s + 1, b).wait_send()
            return carry

        lax.fori_loop(0, chips - 1, drain, 0)

        done(load_wo(layer))
        for n in range(n_out):
            half, off = divmod(n * CHUNK, width)
            sent[0, :, n * CHUNK:(n + 1) * CHUNK] = dot32(avec[...], wqo[half * width:(half + 1) * width, off:off + CHUNK])
            part_hop(layer, 0, n, CHUNK).start()

        @pl.when(layer + 1 < layers)
        def _():
            go(load_wq(layer + 1))

        for n in range(n_out):
            part_hop(layer, 0, n, CHUNK).wait()
        x_mid = (xs[...].astype(jnp.float32) + (sent[0] + got[0])).astype(jnp.bfloat16)
        xs[...] = x_mid

        @pl.when(layer + 1 < layers)
        def _():
            go([page_local(layer + 1, 0), page_local(layer + 1, 1), page_remote(layer + 1, 0), page_remote(layer + 1, 1)])

        hs[...] = rms_norm(xs[...].astype(jnp.float32), gm_ref[layer])

        def gate_up(i, carry):
            slot = lax.rem(layer * n_gu + i, PAIRS)
            done(load_gu(layer, i, slot))
            gate = dot32(hs[...], gu[slot, 0])
            up = dot32(hs[...], gu[slot, 1])
            us[:, pl.ds(gu_start(i), CHUNK)] = (gate * (1.0 / (1.0 + jnp.exp(-gate))) * up).astype(jnp.bfloat16)
            ahead = i + PAIRS

            @pl.when(ahead < n_gu)
            def _():
                go(load_gu(layer, ahead, slot))

            @pl.when(jnp.logical_and(ahead >= n_gu, layer + 1 < layers))
            def _():
                go(load_gu(layer + 1, ahead - n_gu, slot))

            return carry

        lax.fori_loop(0, n_gu, gate_up, 0)

        def down(i, carry):
            slot = lax.rem(layer * n_dn + i, DOWNS)
            done(load_dn(layer, i, slot))
            sent[1, :, pl.ds(pl.multiple_of(i * DOWN, DOWN), DOWN)] = dot32(us[...], dn[slot])
            part_hop(layer, 1, i, DOWN).start()
            ahead = i + DOWNS

            @pl.when(ahead < n_dn)
            def _():
                go(load_dn(layer, ahead, slot))

            @pl.when(jnp.logical_and(ahead >= n_dn, layer + 1 < layers))
            def _():
                go(load_dn(layer + 1, ahead - n_dn, slot))

            return carry

        lax.fori_loop(0, n_dn, down, 0)
        for n in range(n_dn):
            part_hop(layer, 1, n, DOWN).wait()
        xs[...] = (xs[...].astype(jnp.float32) + (sent[1] + got[1])).astype(jnp.bfloat16)
        return carry

    lax.fori_loop(0, layers, layer_body, 0)
    out_ref[...] = xs[own, :]


def solution(mesh):
    group = mesh.shape["pool"]
    by_request = P(("replica", "pool"))
    by_owner = P(None, ("replica", "pool"))
    shared = P()

    def per_device(pool_loc, idx_loc, count_loc, x_loc, norm_attn, wq, wk, wv, wo, norm_mlp, w_gate, w_up, w_down):
        layers, pages, _, page, kv_heads, hd = pool_loc.shape
        slots = idx_loc.shape[2]
        tokens, d_model = x_loc.shape[1:]
        chips = group // 2
        width = wq.shape[2] // 2
        heads = width // hd
        rows = heads * tokens // 2
        ff = w_gate.shape[2] // 2
        both = 2 * tokens

        table = lax.all_gather(jnp.concatenate([idx_loc.reshape(-1), count_loc.reshape(-1)]), "pool")
        k_pages = jnp.transpose(pool_loc[:, :, 0], (0, 3, 1, 2, 4))
        v_pages = jnp.transpose(pool_loc[:, :, 1], (0, 3, 1, 4, 2))
        half = hd // 2
        freqs = ROPE_BASE ** (-jnp.arange(half, dtype=jnp.float32) / half)
        angles = jnp.arange(tokens, dtype=jnp.float32)[:, None] * freqs[None, :]
        cos_t = jnp.tile(jnp.cos(angles), (2, 2))
        sin_t = jnp.tile(jnp.concatenate([-jnp.sin(angles), jnp.sin(angles)], axis=1), (2, 1))

        def gains(one):
            return one.astype(jnp.float32)[:, None]

        vmem = pl.BlockSpec(memory_space=pltpu.VMEM)
        smem = pl.BlockSpec(memory_space=pltpu.SMEM)
        hbm = pl.BlockSpec(memory_space=pl.ANY)
        bf, f32 = jnp.bfloat16, jnp.float32
        dma = pltpu.SemaphoreType.DMA
        n_dn = d_model // DOWN
        out = pl.pallas_call(
            functools.partial(kernel, (group, slots)),
            out_shape=jax.ShapeDtypeStruct((tokens, d_model), bf),
            in_specs=[smem] + [vmem] * 5 + [hbm] * 9,
            out_specs=vmem,
            scratch_shapes=[
                pltpu.VMEM((both, d_model), bf), pltpu.VMEM((both, d_model), bf), pltpu.VMEM((both, width), bf),
                pltpu.VMEM((both, ff), bf),
                pltpu.VMEM((layers, chips, 4, hd, rows), bf), pltpu.VMEM((layers, chips + 1, 4, hd + 8, rows), f32),
                pltpu.VMEM((2, pages, page, hd), bf), pltpu.VMEM((2, pages, hd, page), bf),
                pltpu.VMEM((2, tokens, hd), bf), pltpu.VMEM((2, hd, tokens), bf),
                pltpu.VMEM((2 * slots, page, rows), f32),
                pltpu.VMEM((2, both, d_model), f32), pltpu.VMEM((2, both, d_model), f32),
                pltpu.VMEM((d_model, width), bf), pltpu.VMEM((2, d_model, hd), bf),
                pltpu.VMEM((PAIRS, 2, d_model, CHUNK), bf), pltpu.VMEM((DOWNS, ff, DOWN), bf),
                dma((layers, chips, 4)), dma((layers, chips, 4)), dma((layers, chips, 4)), dma((layers, chips + 1, 4)),
                dma((layers, 2)), dma((layers, 2)), dma((layers, 2)), dma, dma,
                dma((layers, 2, n_dn)), dma((layers, 2, n_dn)),
                dma((3,)), dma((2,)), dma((PAIRS, 2)), dma((DOWNS,)),
            ],
            compiler_params=pltpu.CompilerParams(collective_id=0, has_side_effects=True, vmem_limit_bytes=67000000),
        )(table, x_loc[0], cos_t, sin_t, gains(norm_attn), gains(norm_mlp), k_pages, v_pages, wq, wk, wv, wo, w_gate, w_up, w_down)
        return out[None]

    return jax.shard_map(per_device, mesh=mesh, in_specs=(by_owner, by_owner, by_request, by_request, shared, shared, shared, shared, shared, shared, shared, shared, shared), out_specs=by_request, check_vma=False)
```

```python
import functools

import jax
import jax.numpy as jnp
from jax import lax
from jax.experimental import pallas as pl
from jax.experimental.pallas import tpu as pltpu
from jax.sharding import PartitionSpec as P

EPS = 1e-5
ROPE_BASE = 500000.0
NEG = -1e30
LOG2E = 1.4426950408889634
CHUNK = 512
DOWN = 256
PAIRS = 3
DOWNS = 3
LANDS = 4


def rms_norm(vals_f, gain):
    inv_rms = lax.rsqrt(jnp.mean(vals_f * vals_f, axis=-1, keepdims=True) + EPS)
    return (vals_f * inv_rms * gain).astype(jnp.bfloat16)


def when(cond):
    return lambda body: body() if cond else None


def dot32(a, b):
    return jnp.dot(a, b, preferred_element_type=jnp.float32)


def kernel(dims, meta_ref, x_ref, cos_ref, sin_ref, ga_ref, gm_ref, raw, wq, wk, wv, wo, wg, wu, wd, out_ref,
           xs, hs, avec, us, qbuf, acc, aout, kpgs, vpgs, knew, vnew, scores, sent, got, wqo, wkv, gu, dn,
           metas, tab, land, wide, stage_k, stage_v,
           q_ss, q_rs, a_ss, a_rs, pg_ls, pg_ss, pg_rs, x_ss, x_rs, p_ss, p_rs, wq_s, wkv_s, gu_s, dn_s, m_ss, m_rs, t_s):
    group, slots = dims
    chips = group // 2
    layers, _, d_model = ga_ref.shape
    tokens = x_ref.shape[0]
    hd = raw.shape[-1]
    page = raw.shape[3] // 2
    pages = raw.shape[1]
    width = wq.shape[2] // 2
    heads = width // hd
    part = tokens // 2
    rows = heads * part
    ff = wg.shape[2] // 2
    n_gu = -(-ff // CHUNK)
    n_dn = d_model // DOWN
    n_out = d_model // CHUNK
    share = -(-pages // (chips - 1))
    scale = hd ** -0.5 * LOG2E

    me = lax.axis_index("pool")
    z = me // 2
    c = me % 2
    mate = me + 1 - 2 * c

    def along(b):
        delta = jnp.where(b < 2, 1, chips - 1)
        return lax.rem(z + delta, chips) * 2 + c

    def to(dev):
        return {"pool": dev}

    def q_hop(layer, s, b):
        return pltpu.make_async_remote_copy(
            src_ref=qbuf.at[s, b], dst_ref=qbuf.at[s + 1, b], send_sem=q_ss.at[layer, s, b], recv_sem=q_rs.at[layer, s + 1, b],
            device_id=to(along(b)), device_id_type=pl.DeviceIdType.MESH)

    def a_hop(layer, s, b):
        return pltpu.make_async_remote_copy(
            src_ref=aout.at[lax.rem(s, 2), b], dst_ref=acc.at[s + 1, b], send_sem=a_ss.at[layer, s, b], recv_sem=a_rs.at[layer, s + 1, b],
            device_id=to(along(b)), device_id_type=pl.DeviceIdType.MESH)

    def page_in(layer, pg):
        slot = lax.rem(pg, LANDS)
        return pltpu.make_async_copy(raw.at[layer, pg], land.at[slot], pg_ls.at[slot])

    def page_out(layer, pg):
        slot = lax.rem(pg, LANDS)
        return [pltpu.make_async_remote_copy(
            src_ref=src.at[slot], dst_ref=dst.at[c, pg], send_sem=pg_ss.at[slot, i], recv_sem=pg_rs.at[layer, i],
            device_id=to(mate), device_id_type=pl.DeviceIdType.MESH) for i, (src, dst) in enumerate(((stage_k, kpgs[layer]), (stage_v, vpgs[layer])))]

    def page_arrival(layer):
        return [pltpu.make_async_remote_copy(
            src_ref=dst.at[c], dst_ref=dst.at[1 - c], send_sem=pg_ss.at[0, i], recv_sem=pg_rs.at[layer, i],
            device_id=to(mate), device_id_type=pl.DeviceIdType.MESH) for i, dst in enumerate((kpgs[layer], vpgs[layer]))]

    def prepare(layer, pg):
        slot = lax.rem(pg, LANDS)
        page_in(layer, pg).wait()

        @pl.when(pg >= LANDS)
        def _():
            for one in page_out(layer, pg):
                one.wait_send()

        for kind in range(2):
            wide[kind] = land[slot, kind].astype(jnp.float32)
        mine = pl.ds(c, page, stride=2)
        other = pl.ds(1 - c, page, stride=2)
        kpgs[layer][c, pg] = wide[0, mine, :].astype(jnp.bfloat16)
        stage_k[slot] = wide[0, other, :].astype(jnp.bfloat16)
        vpgs[layer][c, pg] = wide[1, mine, :].T.astype(jnp.bfloat16)
        stage_v[slot] = wide[1, other, :].T.astype(jnp.bfloat16)
        go(page_out(layer, pg))

        @pl.when(pg + LANDS < pages)
        def _():
            page_in(layer, pg + LANDS).start()

    def prepare_end(layer):
        for pg in range(pages - LANDS, pages):
            for one in page_out(layer, pg):
                one.wait_send()

    def meta_hop(off):
        return pltpu.make_async_remote_copy(
            src_ref=meta_ref, dst_ref=metas.at[me], send_sem=m_ss.at[off], recv_sem=m_rs.at[me],
            device_id=to(lax.rem(me + off, group)), device_id_type=pl.DeviceIdType.MESH)

    def meta_arrival(peer):
        return pltpu.make_async_remote_copy(
            src_ref=meta_ref, dst_ref=metas.at[peer], send_sem=m_ss.at[0], recv_sem=m_rs.at[peer],
            device_id=to(mate), device_id_type=pl.DeviceIdType.MESH)

    def part_hop(layer, k, n, size):
        cols = pl.ds(pl.multiple_of(n * size, size), size)
        return pltpu.make_async_remote_copy(
            src_ref=sent.at[k, :, cols], dst_ref=got.at[k, :, cols], send_sem=p_ss.at[layer, k, n], recv_sem=p_rs.at[layer, k, n],
            device_id=to(mate), device_id_type=pl.DeviceIdType.MESH)

    def load_wq(layer):
        cols = pl.ds(pl.multiple_of(c * width, width), width)
        return [pltpu.make_async_copy(wq.at[layer, :, cols], wqo, wq_s.at[0])]

    def load_wkv(layer):
        cols = pl.ds(pl.multiple_of(c * hd, hd), hd)
        return [pltpu.make_async_copy(w.at[layer, :, cols], wkv.at[i], wkv_s.at[i]) for i, w in enumerate((wk, wv))]

    def load_wo(layer):
        line = pl.ds(pl.multiple_of(c * width, width), width)
        return [pltpu.make_async_copy(wo.at[layer, line, pl.ds(i * width, width)], wqo.at[pl.ds(i * width, width), :], wq_s.at[1 + i])
                for i in range(2)]

    def gu_start(i):
        return pl.multiple_of(jnp.minimum(i * CHUNK, ff - CHUNK), 128)

    def load_gu(layer, i, slot):
        cols = pl.ds(pl.multiple_of(c * ff + gu_start(i), 128), CHUNK)
        return [pltpu.make_async_copy(w.at[layer, :, cols], gu.at[slot, j], gu_s.at[slot, j]) for j, w in enumerate((wg, wu))]

    def load_dn(layer, i, slot):
        line = pl.ds(pl.multiple_of(c * ff, 128), ff)
        return [pltpu.make_async_copy(wd.at[layer, line, pl.ds(pl.multiple_of(i * DOWN, DOWN), DOWN)], dn.at[slot], dn_s.at[slot])]

    def go(copies):
        for one in copies:
            one.start()

    def done(copies):
        for one in copies:
            one.wait()

    barrier = pltpu.get_barrier_semaphore()
    for off in range(1, group):
        pl.semaphore_signal(barrier, inc=1, device_id=to(lax.rem(me + off, group)), device_id_type=pl.DeviceIdType.MESH)
    for pg in range(LANDS):
        page_in(0, pg).start()
    go(load_wq(0) + load_wkv(0))
    pl.semaphore_wait(barrier, group - 1)

    own = pl.ds(pl.multiple_of(c * tokens, tokens), tokens)
    x_swap = pltpu.make_async_remote_copy(
        src_ref=x_ref, dst_ref=xs.at[own], send_sem=x_ss, recv_sem=x_rs, device_id=to(mate), device_id_type=pl.DeviceIdType.MESH)
    x_swap.start()
    for off in range(1, group):
        meta_hop(off).start()
    metas[me] = meta_ref[...]
    xs[own, :] = x_ref[...]

    def first(pg, carry):
        prepare(0, pg)
        return carry

    lax.fori_loop(0, pages, first, 0)
    prepare_end(0)
    for i in range(PAIRS):
        go(load_gu(0, i, i))
    for i in range(DOWNS):
        go(load_dn(0, i, i))
    for off in range(1, group):
        meta_hop(off).wait_send()
        meta_arrival(lax.rem(me + off, group)).wait_recv()
    to_tab = pltpu.make_async_copy(metas.at[:, 0, :], tab, t_s)
    to_tab.start()
    to_tab.wait()
    x_swap.wait()
    for pg in range(LANDS):
        page_in(1, pg).start()

    def attend(layer, q_t, req, extra):
        spots = [(o, j) for o in range(2) for j in range(slots)]
        valid, peaks = [], []
        for n, (o, j) in enumerate(spots):
            owner = 2 * z + o
            s = dot32(kpgs[layer][o, tab[owner, req * slots + j]], q_t)
            scores[n] = s
            ok = j < tab[req, group * slots + owner]
            valid.append(ok)
            peaks.append(jnp.where(ok, jnp.max(s, axis=0, keepdims=True) * scale, NEG))
        top = functools.reduce(jnp.maximum, peaks)
        if extra is not None:
            new_s = extra[0]
            top = jnp.maximum(top, jnp.max(new_s, axis=0, keepdims=True) * scale)
        total = jnp.zeros_like(top)
        out = jnp.zeros((hd, rows), jnp.float32)
        for n, (o, j) in enumerate(spots):
            owner = 2 * z + o
            shift = jnp.where(valid[n], -top, NEG)
            p = jnp.exp2(scores[n] * scale + shift)
            total = total + jnp.sum(p, axis=0, keepdims=True)
            out = out + dot32(vpgs[layer][o, tab[owner, req * slots + j]], p.astype(jnp.bfloat16))
        if extra is not None:
            p = jnp.exp2(new_s * scale - top)
            total = total + jnp.sum(p, axis=0, keepdims=True)
            out = out + dot32(extra[1], p.astype(jnp.bfloat16))
        return out, top, total

    def put(ref, out, top, total):
        ref[:hd, :] = out
        line = lax.broadcasted_iota(jnp.int32, (8, rows), 0)
        ref[hd:hd + 8, :] = jnp.where(line == 0, top, total)

    def take(ref):
        return ref[:hd, :], ref[hd:hd + 1, :], ref[hd + 1:hd + 2, :]

    def merge(one, two):
        best = jnp.maximum(one[1], two[1])
        fa, fb = jnp.exp2(one[1] - best), jnp.exp2(two[1] - best)
        return one[0] * fa + two[0] * fb, best, one[2] * fa + two[2] * fb

    def rope(vals):
        return vals * cos_ref[...] + pltpu.roll(vals, hd // 2, axis=1) * sin_ref[...]

    def layer_body(layer, carry):
        last = layer == layers - 1
        hs[...] = rms_norm(xs[...].astype(jnp.float32), ga_ref[layer])
        done(load_wkv(layer))
        k_all = rope(dot32(hs[...], wkv[0])).astype(jnp.bfloat16)
        v_all = dot32(hs[...], wkv[1])
        for i in range(2):
            knew[i] = k_all[i * tokens:(i + 1) * tokens]
            vnew[i] = v_all[i * tokens:(i + 1) * tokens].T.astype(jnp.bfloat16)
        done(load_wq(layer))
        for n in range(heads):
            q_head = rope(dot32(hs[...], wqo[:, n * hd:(n + 1) * hd])).astype(jnp.bfloat16)
            avec[:, n * hd:(n + 1) * hd] = q_head
        for b in range(4):
            lo = (b % 2) * tokens + (b // 2) * part
            q_rows = jnp.concatenate([avec[lo:lo + part, n * hd:(n + 1) * hd] for n in range(heads)], axis=0)
            qbuf[0, b] = q_rows.astype(jnp.float32).T.astype(jnp.bfloat16)
            q_hop(layer, 0, b).start()
        go(load_wo(layer))

        @when(layer + 1 < layers)
        def _():
            go(load_wkv(layer + 1))

        for b in range(4):
            put(acc.at[1, b], jnp.zeros((hd, rows), jnp.float32), jnp.full((1, rows), NEG), jnp.zeros((1, rows), jnp.float32))
        for one in page_arrival(layer):
            one.wait_recv()

        def home(b, carry):
            i = lax.rem(b, 2)
            q_t = qbuf[0, b]
            s = dot32(knew[i], q_t)
            key = lax.broadcasted_iota(jnp.int32, s.shape, 0)
            tok = lax.rem(lax.broadcasted_iota(jnp.int32, s.shape, 1), part) + (b // 2) * part
            s = jnp.where(key <= tok, s, NEG)
            put(acc.at[0, b], *attend(layer, q_t, 2 * z + i, (s, vnew[i])))
            return carry

        lax.fori_loop(0, 4, home, 0)

        def step(s, carry):
            for b in range(4):
                q_hop(layer, s - 1, b).wait_recv()

                @pl.when(s < chips - 1)
                def _():
                    q_hop(layer, s, b).start()

            def block(b, carry):
                source = lax.rem(z + jnp.where(b < 2, chips - s, s), chips)
                found = attend(layer, qbuf[s, b], 2 * source + lax.rem(b, 2), None)

                @pl.when(s >= 2)
                def _():
                    a_hop(layer, s - 1, b).wait_recv()

                @pl.when(s >= 3)
                def _():
                    a_hop(layer, s - 2, b).wait_send()

                @pl.when(s < chips - 1)
                def _():
                    q_hop(layer, s, b).wait_send()

                put(aout.at[lax.rem(s, 2), b], *merge(take(acc.at[s, b]), found))
                a_hop(layer, s, b).start()
                return carry

            lax.fori_loop(0, 4, block, 0)

            @when(layer + 1 < layers)
            def _():
                def one_page(n, carry):
                    prepare(layer + 1, n)
                    return carry

                lax.fori_loop((s - 1) * share, jnp.minimum(s * share, pages), one_page, 0)

            return carry

        lax.fori_loop(1, chips, step, 0)

        @when(layer + 1 < layers)
        def _():
            prepare_end(layer + 1)

        for b in range(4):
            a_hop(layer, chips - 1, b).wait_recv()
            out, top, total = merge(take(acc.at[chips, b]), take(acc.at[0, b]))
            a_rows = (out / total).T.astype(jnp.bfloat16)
            lo = (b % 2) * tokens + (b // 2) * part
            for n in range(heads):
                avec[lo:lo + part, n * hd:(n + 1) * hd] = a_rows[n * part:(n + 1) * part]

        for b in range(4):
            q_hop(layer, 0, b).wait_send()
            a_hop(layer, chips - 2, b).wait_send()
            a_hop(layer, chips - 1, b).wait_send()

        done(load_wo(layer))
        for n in range(n_out):
            half, off = divmod(n * CHUNK, width)
            sent[0, :, n * CHUNK:(n + 1) * CHUNK] = dot32(avec[...], wqo[half * width:(half + 1) * width, off:off + CHUNK])
            part_hop(layer, 0, n, CHUNK).start()

        @when(layer + 1 < layers)
        def _():
            go(load_wq(layer + 1))

        for n in range(n_out):
            part_hop(layer, 0, n, CHUNK).wait()
        x_mid = (xs[...].astype(jnp.float32) + (sent[0] + got[0])).astype(jnp.bfloat16)
        xs[...] = x_mid

        hs[...] = rms_norm(xs[...].astype(jnp.float32), gm_ref[layer])

        def gate_up(i, carry):
            slot = lax.rem(layer * n_gu + i, PAIRS)
            done(load_gu(layer, i, slot))
            gate = dot32(hs[...], gu[slot, 0])
            up = dot32(hs[...], gu[slot, 1])
            us[:, pl.ds(gu_start(i), CHUNK)] = (gate * (1.0 / (1.0 + jnp.exp(-gate))) * up).astype(jnp.bfloat16)
            ahead = i + PAIRS

            @pl.when(ahead < n_gu)
            def _():
                go(load_gu(layer, ahead, slot))

            @pl.when(jnp.logical_and(ahead >= n_gu, layer + 1 < layers))
            def _():
                go(load_gu(min(layer + 1, layers - 1), ahead - n_gu, slot))

            return carry

        lax.fori_loop(0, n_gu, gate_up, 0)

        def down(i, carry):
            slot = lax.rem(layer * n_dn + i, DOWNS)
            done(load_dn(layer, i, slot))
            sent[1, :, pl.ds(pl.multiple_of(i * DOWN, DOWN), DOWN)] = dot32(us[...], dn[slot])
            part_hop(layer, 1, i, DOWN).start()
            ahead = i + DOWNS

            @pl.when(ahead < n_dn)
            def _():
                go(load_dn(layer, ahead, slot))

            @pl.when(jnp.logical_and(ahead >= n_dn, layer + 1 < layers))
            def _():
                go(load_dn(min(layer + 1, layers - 1), ahead - n_dn, slot))

            return carry

        lax.fori_loop(0, n_dn, down, 0)
        for n in range(n_dn):
            part_hop(layer, 1, n, DOWN).wait()
        xs[...] = (xs[...].astype(jnp.float32) + (sent[1] + got[1])).astype(jnp.bfloat16)
        return carry

    for layer in range(layers):
        layer_body(layer, 0)
    out_ref[...] = xs[own, :]


def solution(mesh):
    group = mesh.shape["pool"]
    by_request = P(("replica", "pool"))
    by_owner = P(None, ("replica", "pool"))
    shared = P()

    def per_device(pool_loc, idx_loc, count_loc, x_loc, norm_attn, wq, wk, wv, wo, norm_mlp, w_gate, w_up, w_down):
        layers, pages, _, page, kv_heads, hd = pool_loc.shape
        slots = idx_loc.shape[2]
        tokens, d_model = x_loc.shape[1:]
        chips = group // 2
        width = wq.shape[2] // 2
        heads = width // hd
        rows = heads * tokens // 2
        ff = w_gate.shape[2] // 2
        both = 2 * tokens

        meta = jnp.concatenate([idx_loc.reshape(-1), count_loc.reshape(-1)])
        meta = jnp.broadcast_to(jnp.pad(meta, (0, 128 - meta.shape[0])), (8, 128))
        raw = pool_loc.reshape(layers, pages, 2, page * kv_heads, hd)
        half = hd // 2
        freqs = ROPE_BASE ** (-jnp.arange(half, dtype=jnp.float32) / half)
        angles = jnp.arange(tokens, dtype=jnp.float32)[:, None] * freqs[None, :]
        cos_t = jnp.tile(jnp.cos(angles), (2, 2))
        sin_t = jnp.tile(jnp.concatenate([-jnp.sin(angles), jnp.sin(angles)], axis=1), (2, 1))

        def gains(one):
            return one.astype(jnp.float32)[:, None]

        vmem = pl.BlockSpec(memory_space=pltpu.VMEM)
        hbm = pl.BlockSpec(memory_space=pl.ANY)
        bf, f32 = jnp.bfloat16, jnp.float32
        dma = pltpu.SemaphoreType.DMA
        n_dn = d_model // DOWN
        out = pl.pallas_call(
            functools.partial(kernel, (group, slots)),
            out_shape=jax.ShapeDtypeStruct((tokens, d_model), bf),
            in_specs=[vmem] * 6 + [hbm] * 8,
            out_specs=vmem,
            scratch_shapes=[
                pltpu.VMEM((both, d_model), bf), pltpu.VMEM((both, d_model), bf), pltpu.VMEM((both, width), bf),
                pltpu.VMEM((both, ff), bf),
                pltpu.VMEM((chips, 4, hd, rows), bf), pltpu.VMEM((chips + 1, 4, hd + 8, rows), f32), pltpu.VMEM((2, 4, hd + 8, rows), f32),
                [pltpu.VMEM((2, pages, page, hd), bf)] * layers, [pltpu.VMEM((2, pages, hd, page), bf)] * layers,
                pltpu.VMEM((2, tokens, hd), bf), pltpu.VMEM((2, hd, tokens), bf),
                pltpu.VMEM((2 * slots, page, rows), f32),
                pltpu.VMEM((2, both, d_model), f32), pltpu.VMEM((2, both, d_model), f32),
                pltpu.VMEM((d_model, width), bf), pltpu.VMEM((2, d_model, hd), bf),
                pltpu.VMEM((PAIRS, 2, d_model, CHUNK), bf), pltpu.VMEM((DOWNS, ff, DOWN), bf),
                pltpu.VMEM((group, 8, 128), jnp.int32), pltpu.SMEM((group, 128), jnp.int32),
                pltpu.VMEM((LANDS, 2, 2 * page, hd), bf), pltpu.VMEM((2, 2 * page, hd), f32),
                pltpu.VMEM((LANDS, page, hd), bf), pltpu.VMEM((LANDS, hd, page), bf),
                dma((layers, chips, 4)), dma((layers, chips, 4)), dma((layers, chips, 4)), dma((layers, chips + 1, 4)),
                dma((LANDS,)), dma((LANDS, 2)), dma((layers, 2)), dma, dma,
                dma((layers, 2, n_dn)), dma((layers, 2, n_dn)),
                dma((3,)), dma((2,)), dma((PAIRS, 2)), dma((DOWNS,)),
                dma((group,)), dma((group,)), dma,
            ],
            compiler_params=pltpu.CompilerParams(collective_id=0, has_side_effects=True, vmem_limit_bytes=67000000),
        )(meta, x_loc[0], cos_t, sin_t, gains(norm_attn), gains(norm_mlp), raw, wq, wk, wv, wo, w_gate, w_up, w_down)
        return out[None]

    return jax.shard_map(per_device, mesh=mesh, in_specs=(by_owner, by_owner, by_request, by_request, shared, shared, shared, shared, shared, shared, shared, shared, shared), out_specs=by_request, check_vma=False)
```

```python
import functools

import jax
import jax.numpy as jnp
from jax import lax
from jax.experimental import pallas as pl
from jax.experimental.pallas import tpu as pltpu
from jax.sharding import PartitionSpec as P

EPS = 1e-5
ROPE_BASE = 500000.0
NEG = -1e30
LOG2E = 1.4426950408889634
CHUNK = 512
DOWN = 256
PAIRS = 3
DOWNS = 3
LANDS = 4


def rms_norm(vals_f, gain):
    inv_rms = lax.rsqrt(jnp.mean(vals_f * vals_f, axis=-1, keepdims=True) + EPS)
    return (vals_f * inv_rms * gain).astype(jnp.bfloat16)


def when(cond):
    return lambda body: body() if cond else None


def dot32(a, b):
    return jnp.dot(a, b, preferred_element_type=jnp.float32)


def kernel(dims, meta_ref, x_ref, cos_ref, sin_ref, ga_ref, gm_ref, raw, wq, wk, wv, wo, wg, wu, wd, out_ref,
           xs, hs, avec, qtmp, us, qbuf, acc, aout, found, kpgs, vpgs, knew, vnew, scores, sent, got, wqo, wkv, gu, dn,
           metas, tab, land, wide, stage_k, stage_v,
           q_ss, q_rs, a_ss, a_rs, pg_ls, pg_ss, pg_rs, x_ss, x_rs, p_ss, p_rs, wq_s, wkv_s, gu_s, dn_s, m_ss, m_rs, t_s):
    group, slots = dims
    chips = group // 2
    layers, _, d_model = ga_ref.shape
    tokens = x_ref.shape[0]
    hd = raw.shape[-1]
    page = raw.shape[3] // 2
    pages = raw.shape[1]
    width = wq.shape[2] // 2
    heads = width // hd
    part = tokens // 2
    rows = heads * part
    ff = wg.shape[2] // 2
    n_gu = -(-ff // CHUNK)
    n_dn = d_model // DOWN
    n_out = d_model // CHUNK
    share = -(-pages // (chips - 1))
    scale = hd ** -0.5 * LOG2E
    rings = 2 * layers
    lanes = rows // 2

    me = lax.axis_index("pool")
    z = me // 2
    c = me % 2
    mate = me + 1 - 2 * c

    def along(b):
        delta = jnp.where(b < 1, 1, chips - 1)
        return lax.rem(z + delta, chips) * 2 + c

    def to(dev):
        return {"pool": dev}

    def q_hop(k, s, b):
        return pltpu.make_async_remote_copy(
            src_ref=qbuf.at[k % 2, s, b], dst_ref=qbuf.at[k % 2, s + 1, b], send_sem=q_ss.at[k, s, b], recv_sem=q_rs.at[k, s + 1, b],
            device_id=to(along(b)), device_id_type=pl.DeviceIdType.MESH)

    def a_hop(k, s, b, h):
        return pltpu.make_async_remote_copy(
            src_ref=aout.at[k % 2, lax.rem(s, 2), b, h], dst_ref=acc.at[k % 2, s + 1, b, h],
            send_sem=a_ss.at[k, s, b, h], recv_sem=a_rs.at[k, s + 1, b, h],
            device_id=to(along(b)), device_id_type=pl.DeviceIdType.MESH)

    def page_in(layer, pg):
        slot = lax.rem(pg, LANDS)
        return pltpu.make_async_copy(raw.at[layer, pg], land.at[slot], pg_ls.at[slot])

    def page_out(layer, pg):
        slot = lax.rem(pg, LANDS)
        return [pltpu.make_async_remote_copy(
            src_ref=src.at[slot], dst_ref=dst.at[c, pg], send_sem=pg_ss.at[slot, i], recv_sem=pg_rs.at[layer, i],
            device_id=to(mate), device_id_type=pl.DeviceIdType.MESH) for i, (src, dst) in enumerate(((stage_k, kpgs[layer]), (stage_v, vpgs[layer])))]

    def page_arrival(layer):
        return [pltpu.make_async_remote_copy(
            src_ref=dst.at[c], dst_ref=dst.at[1 - c], send_sem=pg_ss.at[0, i], recv_sem=pg_rs.at[layer, i],
            device_id=to(mate), device_id_type=pl.DeviceIdType.MESH) for i, dst in enumerate((kpgs[layer], vpgs[layer]))]

    def prepare(layer, pg):
        slot = lax.rem(pg, LANDS)
        page_in(layer, pg).wait()

        @pl.when(pg >= LANDS)
        def _():
            for one in page_out(layer, pg):
                one.wait_send()

        for kind in range(2):
            wide[kind] = land[slot, kind].astype(jnp.float32)
        mine = pl.ds(c, page, stride=2)
        other = pl.ds(1 - c, page, stride=2)
        kpgs[layer][c, pg] = wide[0, mine, :].astype(jnp.bfloat16)
        stage_k[slot] = wide[0, other, :].astype(jnp.bfloat16)
        vpgs[layer][c, pg] = wide[1, mine, :].T.astype(jnp.bfloat16)
        stage_v[slot] = wide[1, other, :].T.astype(jnp.bfloat16)
        go(page_out(layer, pg))

        @pl.when(pg + LANDS < pages)
        def _():
            page_in(layer, pg + LANDS).start()

    def prepare_end(layer):
        for pg in range(pages - LANDS, pages):
            for one in page_out(layer, pg):
                one.wait_send()

    def meta_hop(off):
        return pltpu.make_async_remote_copy(
            src_ref=meta_ref, dst_ref=metas.at[me], send_sem=m_ss.at[off], recv_sem=m_rs.at[me],
            device_id=to(lax.rem(me + off, group)), device_id_type=pl.DeviceIdType.MESH)

    def meta_arrival(peer):
        return pltpu.make_async_remote_copy(
            src_ref=meta_ref, dst_ref=metas.at[peer], send_sem=m_ss.at[0], recv_sem=m_rs.at[peer],
            device_id=to(mate), device_id_type=pl.DeviceIdType.MESH)

    def part_hop(k, kind, n, size):
        cols = pl.ds(pl.multiple_of(n * size, size), size)
        return pltpu.make_async_remote_copy(
            src_ref=sent.at[kind, :, cols], dst_ref=got.at[kind, :, cols], send_sem=p_ss.at[k, kind, n], recv_sem=p_rs.at[k, kind, n],
            device_id=to(mate), device_id_type=pl.DeviceIdType.MESH)

    def load_wq(layer):
        cols = pl.ds(pl.multiple_of(c * width, width), width)
        return [pltpu.make_async_copy(wq.at[layer, :, cols], wqo, wq_s.at[0])]

    def load_wkv(layer):
        cols = pl.ds(pl.multiple_of(c * hd, hd), hd)
        return [pltpu.make_async_copy(w.at[layer, :, cols], wkv.at[i], wkv_s.at[i]) for i, w in enumerate((wk, wv))]

    def load_wo(layer):
        line = pl.ds(pl.multiple_of(c * width, width), width)
        return [pltpu.make_async_copy(wo.at[layer, line, pl.ds(i * width, width)], wqo.at[pl.ds(i * width, width), :], wq_s.at[1 + i])
                for i in range(2)]

    def gu_start(i):
        return pl.multiple_of(jnp.minimum(i * CHUNK, ff - CHUNK), 128)

    def load_gu(layer, i, slot):
        cols = pl.ds(pl.multiple_of(c * ff + gu_start(i), 128), CHUNK)
        return [pltpu.make_async_copy(w.at[layer, :, cols], gu.at[slot, j], gu_s.at[slot, j]) for j, w in enumerate((wg, wu))]

    def load_dn(layer, i, slot):
        line = pl.ds(pl.multiple_of(c * ff, 128), ff)
        return [pltpu.make_async_copy(wd.at[layer, line, pl.ds(pl.multiple_of(i * DOWN, DOWN), DOWN)], dn.at[slot], dn_s.at[slot])]

    def go(copies):
        for one in copies:
            one.start()

    def done(copies):
        for one in copies:
            one.wait()

    barrier = pltpu.get_barrier_semaphore()
    for off in range(1, group):
        pl.semaphore_signal(barrier, inc=1, device_id=to(lax.rem(me + off, group)), device_id_type=pl.DeviceIdType.MESH)
    for pg in range(LANDS):
        page_in(0, pg).start()
    go(load_wq(0) + load_wkv(0))
    pl.semaphore_wait(barrier, group - 1)

    own = pl.ds(pl.multiple_of(c * tokens, tokens), tokens)
    x_swap = pltpu.make_async_remote_copy(
        src_ref=x_ref, dst_ref=xs.at[own], send_sem=x_ss, recv_sem=x_rs, device_id=to(mate), device_id_type=pl.DeviceIdType.MESH)
    x_swap.start()
    for off in range(1, group):
        meta_hop(off).start()
    metas[me] = meta_ref[...]
    xs[own, :] = x_ref[...]

    def first(pg, carry):
        prepare(0, pg)
        return carry

    lax.fori_loop(0, pages, first, 0)
    prepare_end(0)
    for i in range(PAIRS):
        go(load_gu(0, i, i))
    for i in range(DOWNS):
        go(load_dn(0, i, i))
    for off in range(1, group):
        meta_hop(off).wait_send()
        meta_arrival(lax.rem(me + off, group)).wait_recv()
    to_tab = pltpu.make_async_copy(metas.at[:, 0, :], tab, t_s)
    to_tab.start()
    to_tab.wait()
    x_swap.wait()
    def attend(layer, q_t, req, extra):
        spots = [(o, j) for o in range(2) for j in range(slots)]
        valid, peaks = [], []
        for n, (o, j) in enumerate(spots):
            owner = 2 * z + o
            s = dot32(kpgs[layer][o, tab[owner, req * slots + j]], q_t)
            scores[n] = s
            ok = j < tab[req, group * slots + owner]
            valid.append(ok)
            peaks.append(jnp.where(ok, jnp.max(s, axis=0, keepdims=True) * scale, NEG))
        top = functools.reduce(jnp.maximum, peaks)
        if extra is not None:
            new_s = extra[0]
            top = jnp.maximum(top, jnp.max(new_s, axis=0, keepdims=True) * scale)
        total = jnp.zeros_like(top)
        out = jnp.zeros((hd, rows), jnp.float32)
        for n, (o, j) in enumerate(spots):
            owner = 2 * z + o
            shift = jnp.where(valid[n], -top, NEG)
            p = jnp.exp2(scores[n] * scale + shift)
            total = total + jnp.sum(p, axis=0, keepdims=True)
            out = out + dot32(vpgs[layer][o, tab[owner, req * slots + j]], p.astype(jnp.bfloat16))
        if extra is not None:
            p = jnp.exp2(new_s * scale - top)
            total = total + jnp.sum(p, axis=0, keepdims=True)
            out = out + dot32(extra[1], p.astype(jnp.bfloat16))
        return out, top, total

    def put(ref, out, top, total):
        line = lax.broadcasted_iota(jnp.int32, (8, rows), 0)
        tail = jnp.where(line == 0, top, total)
        for h in range(2):
            ref[h, :hd, :] = out[:, h * lanes:(h + 1) * lanes]
            ref[h, hd:hd + 8, :] = tail[:, h * lanes:(h + 1) * lanes]

    def take(ref):
        return ref[:hd, :], ref[hd:hd + 1, :], ref[hd + 1:hd + 2, :]

    def merge(one, two):
        best = jnp.maximum(one[1], two[1])
        fa, fb = jnp.exp2(one[1] - best), jnp.exp2(two[1] - best)
        return one[0] * fa + two[0] * fb, best, one[2] * fa + two[2] * fb

    def rope(vals):
        return vals * cos_ref[:vals.shape[0]] + pltpu.roll(vals, hd // 2, axis=1) * sin_ref[:vals.shape[0]]

    def project(layer, streams):
        first, count = streams[0] * tokens, len(streams) * tokens
        hs[:count] = rms_norm(xs[first:first + count].astype(jnp.float32), ga_ref[layer])
        h_all = hs[:count]
        k_all = rope(dot32(h_all, wkv[0])).astype(jnp.bfloat16)
        v_all = dot32(h_all, wkv[1])
        for n, i in enumerate(streams):
            knew[i] = k_all[n * tokens:(n + 1) * tokens]
            vnew[i] = v_all[n * tokens:(n + 1) * tokens].T.astype(jnp.bfloat16)
        done(load_wq(layer))
        for n in range(heads):
            qtmp[:count, n * hd:(n + 1) * hd] = rope(dot32(h_all, wqo[:, n * hd:(n + 1) * hd])).astype(jnp.bfloat16)
        for n, i in enumerate(streams):
            for b in range(2):
                lo = n * tokens + b * part
                q_rows = jnp.concatenate([qtmp[lo:lo + part, m * hd:(m + 1) * hd] for m in range(heads)], axis=0)
                qbuf[i, 0, b] = q_rows.astype(jnp.float32).T.astype(jnp.bfloat16)

    def finish(k):
        i = k % 2
        for b in range(2):
            for h in range(2):
                a_hop(k, chips - 1, b, h).wait_recv()
                out, top, total = merge(take(acc.at[i, chips, b, h]), take(acc.at[i, 0, b, h]))
                a_rows = (out / total).T.astype(jnp.bfloat16)
                for n in range(lanes // part):
                    head = h * (lanes // part) + n
                    avec[b * part:(b + 1) * part, head * hd:(head + 1) * hd] = a_rows[n * part:(n + 1) * part]
        for b in range(2):
            q_hop(k, 0, b).wait_send()
            for h in range(2):
                a_hop(k, chips - 2, b, h).wait_send()
                a_hop(k, chips - 1, b, h).wait_send()
        done(load_wo(k // 2))
        for n in range(n_out):
            half, off = divmod(n * CHUNK, width)
            sent[0, :, n * CHUNK:(n + 1) * CHUNK] = dot32(avec[...], wqo[half * width:(half + 1) * width, off:off + CHUNK])
            part_hop(k, 0, n, CHUNK).start()
        if k // 2 + 1 < layers:
            go(load_wq(k // 2 + 1))
        elif k + 1 < rings:
            go(load_wo((k + 1) // 2))

    def middle(k):
        mine = slice((k % 2) * tokens, (k % 2 + 1) * tokens)
        for n in range(n_out):
            part_hop(k, 0, n, CHUNK).wait()
        xs[mine] = (xs[mine].astype(jnp.float32) + (sent[0] + got[0])).astype(jnp.bfloat16)
        hs[:tokens] = rms_norm(xs[mine].astype(jnp.float32), gm_ref[k // 2])

    def gate_up(k, lo, hi):
        def body(i, carry):
            slot = lax.rem(k * n_gu + i, PAIRS)
            done(load_gu(k // 2, i, slot))
            gate = dot32(hs[:tokens], gu[slot, 0])
            up = dot32(hs[:tokens], gu[slot, 1])
            us[:, pl.ds(gu_start(i), CHUNK)] = (gate * (1.0 / (1.0 + jnp.exp(-gate))) * up).astype(jnp.bfloat16)
            ahead = i + PAIRS

            @pl.when(ahead < n_gu)
            def _():
                go(load_gu(k // 2, ahead, slot))

            if k + 1 < rings:
                @pl.when(ahead >= n_gu)
                def _():
                    go(load_gu((k + 1) // 2, ahead - n_gu, slot))

            return carry

        lax.fori_loop(lo, hi, body, 0)

    def down(k, lo, hi):
        def body(i, carry):
            slot = lax.rem(k * n_dn + i, DOWNS)
            done(load_dn(k // 2, i, slot))
            sent[1, :, pl.ds(pl.multiple_of(i * DOWN, DOWN), DOWN)] = dot32(us[...], dn[slot])
            part_hop(k, 1, i, DOWN).start()
            ahead = i + DOWNS

            @pl.when(ahead < n_dn)
            def _():
                go(load_dn(k // 2, ahead, slot))

            if k + 1 < rings:
                @pl.when(ahead >= n_dn)
                def _():
                    go(load_dn((k + 1) // 2, ahead - n_dn, slot))

            return carry

        lax.fori_loop(lo, hi, body, 0)

    def close(k):
        mine = slice((k % 2) * tokens, (k % 2 + 1) * tokens)
        for n in range(n_dn):
            part_hop(k, 1, n, DOWN).wait()
        xs[mine] = (xs[mine].astype(jnp.float32) + (sent[1] + got[1])).astype(jnp.bfloat16)
        if k // 2 + 1 < layers:
            if k % 2 == 0:
                done(load_wkv(k // 2 + 1))
            project(k // 2 + 1, (k % 2,))
            go(load_wo((k + 1) // 2))
            if k % 2 == 1 and k // 2 + 2 < layers:
                go(load_wkv(k // 2 + 2))
            for b in range(2):
                q_hop(k + 2, 0, b).start()

    def follow(k, s):
        steps = chips - 1
        up_steps = steps // 2
        per_up = -(-n_gu // up_steps)
        down_steps = steps - 2 - up_steps
        per_down = -(-n_dn // down_steps)

        @pl.when(s == 1)
        def _():
            finish(k)

        @pl.when(s == 2)
        def _():
            middle(k)

        up_lo = jnp.clip((s - 2) * per_up, 0, n_gu)
        gate_up(k, up_lo, jnp.where(s >= 2, jnp.clip((s - 1) * per_up, 0, n_gu), up_lo))
        at = s - 2 - up_steps
        down_lo = jnp.clip(at * per_down, 0, n_dn)
        down(k, down_lo, jnp.where(at >= 0, jnp.clip((at + 1) * per_down, 0, n_dn), down_lo))

        @pl.when(s == steps)
        def _():
            close(k)

    def ring(k):
        layer, i = divmod(k, 2)
        for b in range(2):
            for h in range(2):
                acc[i, 1, b, h, :, :] = jnp.where(lax.broadcasted_iota(jnp.int32, (hd + 8, lanes), 0) == hd, NEG, 0.0)
        if i == 0:
            for one in page_arrival(layer):
                one.wait_recv()

        def home(b, carry):
            q_t = qbuf[i, 0, b]
            s = dot32(knew[i], q_t)
            key = lax.broadcasted_iota(jnp.int32, s.shape, 0)
            tok = lax.rem(lax.broadcasted_iota(jnp.int32, s.shape, 1), part) + b * part
            s = jnp.where(key <= tok, s, NEG)
            put(acc.at[i, 0, b], *attend(layer, q_t, 2 * z + i, (s, vnew[i])))
            return carry

        lax.fori_loop(0, 2, home, 0)

        def step(s, carry):
            for b in range(2):
                q_hop(k, s - 1, b).wait_recv()

                @pl.when(s < chips - 1)
                def _():
                    q_hop(k, s, b).start()

            def block(b, carry):
                source = lax.rem(z + jnp.where(b < 1, chips - s, s), chips)
                put(found.at[b], *attend(layer, qbuf[i, s, b], 2 * source + i, None))
                return carry

            lax.fori_loop(0, 2, block, 0)
            if k > 0:
                follow(k - 1, s)
            else:
                if layers > 1:
                    def one_page(n, carry):
                        prepare(1, n)
                        return carry

                    lax.fori_loop((s - 1) * share, jnp.minimum(s * share, pages), one_page, 0)

                @pl.when(s == chips - 1)
                def _():
                    for b in range(2):
                        q_hop(1, 0, b).start()

            @pl.when(s < chips - 1)
            def _():
                for b in range(2):
                    q_hop(k, s, b).wait_send()

            def pass_on(n, carry):
                h, b = n // 2, lax.rem(n, 2)

                @pl.when(s >= 2)
                def _():
                    a_hop(k, s - 1, b, h).wait_recv()

                @pl.when(s >= 3)
                def _():
                    a_hop(k, s - 2, b, h).wait_send()

                out, top, total = merge(take(acc.at[i, s, b, h]), take(found.at[b, h]))
                slot = lax.rem(s, 2)
                aout[i, slot, b, h, :hd, :] = out
                line = lax.broadcasted_iota(jnp.int32, (8, lanes), 0)
                aout[i, slot, b, h, hd:hd + 8, :] = jnp.where(line == 0, top, total)
                a_hop(k, s, b, h).start()
                return carry

            return lax.fori_loop(0, 4, pass_on, carry)

        lax.fori_loop(1, chips, step, 0)
        if k == 0 and layers > 1:
            prepare_end(1)

    done(load_wkv(0))
    project(0, (0, 1))
    for b in range(2):
        q_hop(0, 0, b).start()
    go(load_wo(0))
    if layers > 1:
        go(load_wkv(1))
        for pg in range(LANDS):
            page_in(1, pg).start()
    for k in range(rings):
        ring(k)
    k = rings - 1
    finish(k)
    middle(k)
    gate_up(k, 0, n_gu)
    down(k, 0, n_dn)
    close(k)
    out_ref[...] = xs[own, :]


def solution(mesh):
    group = mesh.shape["pool"]
    by_request = P(("replica", "pool"))
    by_owner = P(None, ("replica", "pool"))
    shared = P()

    def per_device(pool_loc, idx_loc, count_loc, x_loc, norm_attn, wq, wk, wv, wo, norm_mlp, w_gate, w_up, w_down):
        layers, pages, _, page, kv_heads, hd = pool_loc.shape
        slots = idx_loc.shape[2]
        tokens, d_model = x_loc.shape[1:]
        chips = group // 2
        width = wq.shape[2] // 2
        heads = width // hd
        rows = heads * tokens // 2
        ff = w_gate.shape[2] // 2
        both = 2 * tokens
        rings = 2 * layers

        meta = jnp.concatenate([idx_loc.reshape(-1), count_loc.reshape(-1)])
        meta = jnp.broadcast_to(jnp.pad(meta, (0, 128 - meta.shape[0])), (8, 128))
        raw = pool_loc.reshape(layers, pages, 2, page * kv_heads, hd)
        half = hd // 2
        freqs = ROPE_BASE ** (-jnp.arange(half, dtype=jnp.float32) / half)
        angles = jnp.arange(tokens, dtype=jnp.float32)[:, None] * freqs[None, :]
        cos_t = jnp.tile(jnp.cos(angles), (2, 2))
        sin_t = jnp.tile(jnp.concatenate([-jnp.sin(angles), jnp.sin(angles)], axis=1), (2, 1))

        def gains(one):
            return one.astype(jnp.float32)[:, None]

        vmem = pl.BlockSpec(memory_space=pltpu.VMEM)
        hbm = pl.BlockSpec(memory_space=pl.ANY)
        bf, f32 = jnp.bfloat16, jnp.float32
        dma = pltpu.SemaphoreType.DMA
        n_dn = d_model // DOWN
        out = pl.pallas_call(
            functools.partial(kernel, (group, slots)),
            out_shape=jax.ShapeDtypeStruct((tokens, d_model), bf),
            in_specs=[vmem] * 6 + [hbm] * 8,
            out_specs=vmem,
            scratch_shapes=[
                pltpu.VMEM((both, d_model), bf), pltpu.VMEM((both, d_model), bf), pltpu.VMEM((tokens, width), bf), pltpu.VMEM((both, width), bf),
                pltpu.VMEM((tokens, ff), bf),
                pltpu.VMEM((2, chips, 2, hd, rows), bf), pltpu.VMEM((2, chips + 1, 2, 2, hd + 8, rows // 2), f32),
                pltpu.VMEM((2, 2, 2, 2, hd + 8, rows // 2), f32), pltpu.VMEM((2, 2, hd + 8, rows // 2), f32),
                [pltpu.VMEM((2, pages, page, hd), bf)] * layers, [pltpu.VMEM((2, pages, hd, page), bf)] * layers,
                pltpu.VMEM((2, tokens, hd), bf), pltpu.VMEM((2, hd, tokens), bf),
                pltpu.VMEM((2 * slots, page, rows), f32),
                pltpu.VMEM((2, tokens, d_model), f32), pltpu.VMEM((2, tokens, d_model), f32),
                pltpu.VMEM((d_model, width), bf), pltpu.VMEM((2, d_model, hd), bf),
                pltpu.VMEM((PAIRS, 2, d_model, CHUNK), bf), pltpu.VMEM((DOWNS, ff, DOWN), bf),
                pltpu.VMEM((group, 8, 128), jnp.int32), pltpu.SMEM((group, 128), jnp.int32),
                pltpu.VMEM((LANDS, 2, 2 * page, hd), bf), pltpu.VMEM((2, 2 * page, hd), f32),
                pltpu.VMEM((LANDS, page, hd), bf), pltpu.VMEM((LANDS, hd, page), bf),
                dma((rings, chips, 2)), dma((rings, chips, 2)), dma((rings, chips, 2, 2)), dma((rings, chips + 1, 2, 2)),
                dma((LANDS,)), dma((LANDS, 2)), dma((layers, 2)), dma, dma,
                dma((rings, 2, n_dn)), dma((rings, 2, n_dn)),
                dma((3,)), dma((2,)), dma((PAIRS, 2)), dma((DOWNS,)),
                dma((group,)), dma((group,)), dma,
            ],
            compiler_params=pltpu.CompilerParams(collective_id=0, has_side_effects=True, vmem_limit_bytes=67000000),
        )(meta, x_loc[0], cos_t, sin_t, gains(norm_attn), gains(norm_mlp), raw, wq, wk, wv, wo, w_gate, w_up, w_down)
        return out[None]

    return jax.shard_map(per_device, mesh=mesh, in_specs=(by_owner, by_owner, by_request, by_request, shared, shared, shared, shared, shared, shared, shared, shared, shared), out_specs=by_request, check_vma=False)
```

```python
import functools

import jax
import jax.numpy as jnp
from jax import lax
from jax.experimental import pallas as pl
from jax.experimental.pallas import tpu as pltpu
from jax.sharding import PartitionSpec as P

EPS = 1e-5
ROPE_BASE = 500000.0
NEG = -1e30
LOG2E = 1.4426950408889634
CHUNK = 512
DOWN = 256
PAIRS = 3
DOWNS = 3
LANDS = 4


def rms_norm(vals_f, gain):
    inv_rms = lax.rsqrt(jnp.mean(vals_f * vals_f, axis=-1, keepdims=True) + EPS)
    return (vals_f * inv_rms * gain).astype(jnp.bfloat16)


def when(cond):
    return lambda body: body() if cond else None


def dot32(a, b):
    return jnp.dot(a, b, preferred_element_type=jnp.float32)


def kernel(dims, meta_ref, x_ref, cos_ref, sin_ref, ga_ref, gm_ref, raw, wq, wk, wv, wo, wg, wu, wd, out_ref,
           xs, hs, avec, qtmp, us, qbuf, acc, aout, found, kpgs, vpgs, knew, vnew, scores, sent, got, wqo, wkv, gu, dn,
           metas, tab, land, wide, stage_k, stage_v,
           q_ss, q_rs, a_ss, a_rs, pg_ls, pg_ss, pg_rs, x_ss, x_rs, p_ss, p_rs, wq_s, wkv_s, gu_s, dn_s, m_ss, m_rs, t_s):
    group, slots = dims
    chips = group // 2
    layers, _, d_model = ga_ref.shape
    tokens = x_ref.shape[0]
    hd = raw.shape[-1]
    page = raw.shape[3] // 2
    pages = raw.shape[1]
    width = wq.shape[2] // 2
    heads = width // hd
    part = tokens // 2
    rows = heads * part
    ff = wg.shape[2] // 2
    n_gu = -(-ff // CHUNK)
    n_dn = d_model // DOWN
    n_out = d_model // CHUNK
    share = -(-pages // (chips - 1))
    scale = hd ** -0.5 * LOG2E
    rings = 2 * layers
    lanes = rows // 2

    me = lax.axis_index("pool")
    z = me // 2
    c = me % 2
    mate = me + 1 - 2 * c

    def along(b):
        delta = jnp.where(b < 1, 1, chips - 1)
        return lax.rem(z + delta, chips) * 2 + c

    def to(dev):
        return {"pool": dev}

    def q_hop(k, s, b):
        return pltpu.make_async_remote_copy(
            src_ref=qbuf.at[k % 2, s, b], dst_ref=qbuf.at[k % 2, s + 1, b], send_sem=q_ss.at[k, s, b], recv_sem=q_rs.at[k, s + 1, b],
            device_id=to(along(b)), device_id_type=pl.DeviceIdType.MESH)

    def a_hop(k, s, b, h):
        return pltpu.make_async_remote_copy(
            src_ref=aout.at[k % 2, lax.rem(s, 2), b, h], dst_ref=acc.at[k % 2, s + 1, b, h],
            send_sem=a_ss.at[k, s, b, h], recv_sem=a_rs.at[k, s + 1, b, h],
            device_id=to(along(b)), device_id_type=pl.DeviceIdType.MESH)

    def page_in(layer, pg):
        slot = lax.rem(pg, LANDS)
        return pltpu.make_async_copy(raw.at[layer, pg], land.at[slot], pg_ls.at[slot])

    def page_out(layer, pg):
        slot = lax.rem(pg, LANDS)
        return [pltpu.make_async_remote_copy(
            src_ref=src.at[slot], dst_ref=dst.at[c, pg], send_sem=pg_ss.at[slot, i], recv_sem=pg_rs.at[layer, i],
            device_id=to(mate), device_id_type=pl.DeviceIdType.MESH) for i, (src, dst) in enumerate(((stage_k, kpgs[layer]), (stage_v, vpgs[layer])))]

    def page_arrival(layer):
        return [pltpu.make_async_remote_copy(
            src_ref=dst.at[c], dst_ref=dst.at[1 - c], send_sem=pg_ss.at[0, i], recv_sem=pg_rs.at[layer, i],
            device_id=to(mate), device_id_type=pl.DeviceIdType.MESH) for i, dst in enumerate((kpgs[layer], vpgs[layer]))]

    def prepare(layer, pg):
        slot = lax.rem(pg, LANDS)
        page_in(layer, pg).wait()

        @pl.when(pg >= LANDS)
        def _():
            for one in page_out(layer, pg):
                one.wait_send()

        for kind in range(2):
            wide[kind] = land[slot, kind].astype(jnp.float32)
        mine = pl.ds(c, page, stride=2)
        other = pl.ds(1 - c, page, stride=2)
        kpgs[layer][c, pg] = wide[0, mine, :].astype(jnp.bfloat16)
        stage_k[slot] = wide[0, other, :].astype(jnp.bfloat16)
        vpgs[layer][c, pg] = wide[1, mine, :].T.astype(jnp.bfloat16)
        stage_v[slot] = wide[1, other, :].T.astype(jnp.bfloat16)
        go(page_out(layer, pg))

        @pl.when(pg + LANDS < pages)
        def _():
            page_in(layer, pg + LANDS).start()

    def prepare_end(layer):
        for pg in range(pages - LANDS, pages):
            for one in page_out(layer, pg):
                one.wait_send()

    def meta_hop(off):
        return pltpu.make_async_remote_copy(
            src_ref=meta_ref, dst_ref=metas.at[me], send_sem=m_ss.at[off], recv_sem=m_rs.at[me],
            device_id=to(lax.rem(me + off, group)), device_id_type=pl.DeviceIdType.MESH)

    def meta_arrival(peer):
        return pltpu.make_async_remote_copy(
            src_ref=meta_ref, dst_ref=metas.at[peer], send_sem=m_ss.at[0], recv_sem=m_rs.at[peer],
            device_id=to(mate), device_id_type=pl.DeviceIdType.MESH)

    def part_hop(k, kind, n, size):
        cols = pl.ds(pl.multiple_of(n * size, size), size)
        return pltpu.make_async_remote_copy(
            src_ref=sent.at[kind, :, cols], dst_ref=got.at[kind, :, cols], send_sem=p_ss.at[k, kind, n], recv_sem=p_rs.at[k, kind, n],
            device_id=to(mate), device_id_type=pl.DeviceIdType.MESH)

    def load_wq(layer):
        cols = pl.ds(pl.multiple_of(c * width, width), width)
        return [pltpu.make_async_copy(wq.at[layer, :, cols], wqo, wq_s.at[0])]

    def load_wkv(layer):
        cols = pl.ds(pl.multiple_of(c * hd, hd), hd)
        return [pltpu.make_async_copy(w.at[layer, :, cols], wkv.at[i], wkv_s.at[i]) for i, w in enumerate((wk, wv))]

    def load_wo(layer):
        line = pl.ds(pl.multiple_of(c * width, width), width)
        return [pltpu.make_async_copy(wo.at[layer, line, pl.ds(i * width, width)], wqo.at[pl.ds(i * width, width), :], wq_s.at[1 + i])
                for i in range(2)]

    def gu_start(i):
        return pl.multiple_of(jnp.minimum(i * CHUNK, ff - CHUNK), 128)

    def load_gu(layer, i, slot):
        cols = pl.ds(pl.multiple_of(c * ff + gu_start(i), 128), CHUNK)
        return [pltpu.make_async_copy(w.at[layer, :, cols], gu.at[slot, j], gu_s.at[slot, j]) for j, w in enumerate((wg, wu))]

    def load_dn(layer, i, slot):
        line = pl.ds(pl.multiple_of(c * ff, 128), ff)
        return [pltpu.make_async_copy(wd.at[layer, line, pl.ds(pl.multiple_of(i * DOWN, DOWN), DOWN)], dn.at[slot], dn_s.at[slot])]

    def go(copies):
        for one in copies:
            one.start()

    def done(copies):
        for one in copies:
            one.wait()

    barrier = pltpu.get_barrier_semaphore()
    for off in range(1, group):
        pl.semaphore_signal(barrier, inc=1, device_id=to(lax.rem(me + off, group)), device_id_type=pl.DeviceIdType.MESH)
    for pg in range(LANDS):
        page_in(0, pg).start()
    go(load_wq(0) + load_wkv(0))
    pl.semaphore_wait(barrier, group - 1)

    own = pl.ds(pl.multiple_of(c * tokens, tokens), tokens)
    x_swap = pltpu.make_async_remote_copy(
        src_ref=x_ref, dst_ref=xs.at[own], send_sem=x_ss, recv_sem=x_rs, device_id=to(mate), device_id_type=pl.DeviceIdType.MESH)
    x_swap.start()
    for off in range(1, group):
        meta_hop(off).start()
    metas[me] = meta_ref[...]
    xs[own, :] = x_ref[...]

    def first(pg, carry):
        prepare(0, pg)
        return carry

    lax.fori_loop(0, pages, first, 0)
    prepare_end(0)
    for i in range(PAIRS):
        go(load_gu(0, i, i))
    for i in range(DOWNS):
        go(load_dn(0, i, i))
    for off in range(1, group):
        meta_hop(off).wait_send()
        meta_arrival(lax.rem(me + off, group)).wait_recv()
    to_tab = pltpu.make_async_copy(metas.at[:, 0, :], tab, t_s)
    to_tab.start()
    to_tab.wait()
    x_swap.wait()
    def attend(layer, q_t, req, extra):
        spots = [(o, j) for o in range(2) for j in range(slots)]
        valid, peaks = [], []
        for n, (o, j) in enumerate(spots):
            owner = 2 * z + o
            s = dot32(kpgs[layer][o, tab[owner, req * slots + j]], q_t)
            scores[n] = s
            ok = j < tab[req, group * slots + owner]
            valid.append(ok)
            peaks.append(jnp.where(ok, jnp.max(s, axis=0, keepdims=True) * scale, NEG))
        top = functools.reduce(jnp.maximum, peaks)
        if extra is not None:
            new_s = extra[0]
            top = jnp.maximum(top, jnp.max(new_s, axis=0, keepdims=True) * scale)
        total = jnp.zeros_like(top)
        out = jnp.zeros((hd, rows), jnp.float32)
        for n, (o, j) in enumerate(spots):
            owner = 2 * z + o
            shift = jnp.where(valid[n], -top, NEG)
            p = jnp.exp2(scores[n] * scale + shift)
            total = total + jnp.sum(p, axis=0, keepdims=True)
            out = out + dot32(vpgs[layer][o, tab[owner, req * slots + j]], p.astype(jnp.bfloat16))
        if extra is not None:
            p = jnp.exp2(new_s * scale - top)
            total = total + jnp.sum(p, axis=0, keepdims=True)
            out = out + dot32(extra[1], p.astype(jnp.bfloat16))
        return out, top, total

    def put(ref, out, top, total):
        line = lax.broadcasted_iota(jnp.int32, (8, rows), 0)
        tail = jnp.where(line == 0, top, total)
        for h in range(2):
            ref[h, :hd, :] = out[:, h * lanes:(h + 1) * lanes]
            ref[h, hd:hd + 8, :] = tail[:, h * lanes:(h + 1) * lanes]

    def take(ref):
        return ref[:hd, :], ref[hd:hd + 1, :], ref[hd + 1:hd + 2, :]

    def merge(one, two):
        best = jnp.maximum(one[1], two[1])
        fa, fb = jnp.exp2(one[1] - best), jnp.exp2(two[1] - best)
        return one[0] * fa + two[0] * fb, best, one[2] * fa + two[2] * fb

    def rope(vals):
        return vals * cos_ref[:vals.shape[0]] + pltpu.roll(vals, hd // 2, axis=1) * sin_ref[:vals.shape[0]]

    def project(layer, streams):
        first, count = streams[0] * tokens, len(streams) * tokens
        hs[:count] = rms_norm(xs[first:first + count].astype(jnp.float32), ga_ref[layer])
        h_all = hs[:count]
        k_all = rope(dot32(h_all, wkv[0])).astype(jnp.bfloat16)
        v_all = dot32(h_all, wkv[1])
        for n, i in enumerate(streams):
            knew[i] = k_all[n * tokens:(n + 1) * tokens]
            vnew[i] = v_all[n * tokens:(n + 1) * tokens].T.astype(jnp.bfloat16)
        done(load_wq(layer))
        for n in range(heads):
            qtmp[:count, n * hd:(n + 1) * hd] = rope(dot32(h_all, wqo[:, n * hd:(n + 1) * hd])).astype(jnp.bfloat16)
        for n, i in enumerate(streams):
            for b in range(2):
                lo = n * tokens + b * part
                q_rows = jnp.concatenate([qtmp[lo:lo + part, m * hd:(m + 1) * hd] for m in range(heads)], axis=0)
                qbuf[i, 0, b] = q_rows.astype(jnp.float32).T.astype(jnp.bfloat16)

    def finish(k):
        i = k % 2
        for b in range(2):
            for h in range(2):
                a_hop(k, chips - 1, b, h).wait_recv()
                out, top, total = merge(take(acc.at[i, chips, b, h]), take(acc.at[i, 0, b, h]))
                a_rows = (out / total).T.astype(jnp.bfloat16)
                for n in range(lanes // part):
                    head = h * (lanes // part) + n
                    avec[b * part:(b + 1) * part, head * hd:(head + 1) * hd] = a_rows[n * part:(n + 1) * part]
        for b in range(2):
            q_hop(k, 0, b).wait_send()
            for h in range(2):
                a_hop(k, chips - 2, b, h).wait_send()
                a_hop(k, chips - 1, b, h).wait_send()
        done(load_wo(k // 2))
        for n in range(n_out):
            half, off = divmod(n * CHUNK, width)
            sent[0, :, n * CHUNK:(n + 1) * CHUNK] = dot32(avec[...], wqo[half * width:(half + 1) * width, off:off + CHUNK])
            part_hop(k, 0, n, CHUNK).start()
        if k // 2 + 1 < layers:
            go(load_wq(k // 2 + 1))
        elif k + 1 < rings:
            go(load_wo((k + 1) // 2))

    def middle(k):
        mine = slice((k % 2) * tokens, (k % 2 + 1) * tokens)
        for n in range(n_out):
            part_hop(k, 0, n, CHUNK).wait()
        xs[mine] = (xs[mine].astype(jnp.float32) + (sent[0] + got[0])).astype(jnp.bfloat16)
        hs[:tokens] = rms_norm(xs[mine].astype(jnp.float32), gm_ref[k // 2])

    def gate_up(k, lo, hi):
        def body(i, carry):
            slot = lax.rem(k * n_gu + i, PAIRS)
            done(load_gu(k // 2, i, slot))
            gate = dot32(hs[:tokens], gu[slot, 0])
            up = dot32(hs[:tokens], gu[slot, 1])
            us[:, pl.ds(gu_start(i), CHUNK)] = (gate * (1.0 / (1.0 + jnp.exp(-gate))) * up).astype(jnp.bfloat16)
            ahead = i + PAIRS

            @pl.when(ahead < n_gu)
            def _():
                go(load_gu(k // 2, ahead, slot))

            if k + 1 < rings:
                @pl.when(ahead >= n_gu)
                def _():
                    go(load_gu((k + 1) // 2, ahead - n_gu, slot))

            return carry

        lax.fori_loop(lo, hi, body, 0)

    def down(k, lo, hi):
        def body(i, carry):
            slot = lax.rem(k * n_dn + i, DOWNS)
            done(load_dn(k // 2, i, slot))
            sent[1, :, pl.ds(pl.multiple_of(i * DOWN, DOWN), DOWN)] = dot32(us[...], dn[slot])
            part_hop(k, 1, i, DOWN).start()
            ahead = i + DOWNS

            @pl.when(ahead < n_dn)
            def _():
                go(load_dn(k // 2, ahead, slot))

            if k + 1 < rings:
                @pl.when(ahead >= n_dn)
                def _():
                    go(load_dn((k + 1) // 2, ahead - n_dn, slot))

            return carry

        lax.fori_loop(lo, hi, body, 0)

    def close(k):
        mine = slice((k % 2) * tokens, (k % 2 + 1) * tokens)
        for n in range(n_dn):
            part_hop(k, 1, n, DOWN).wait()
        xs[mine] = (xs[mine].astype(jnp.float32) + (sent[1] + got[1])).astype(jnp.bfloat16)
        if k // 2 + 1 < layers:
            if k % 2 == 0:
                done(load_wkv(k // 2 + 1))
            project(k // 2 + 1, (k % 2,))
            go(load_wo((k + 1) // 2))
            if k % 2 == 1 and k // 2 + 2 < layers:
                go(load_wkv(k // 2 + 2))
            for b in range(2):
                q_hop(k + 2, 0, b).start()

    def follow(k, s):
        steps = chips - 1
        up_steps = steps // 2
        per_up = -(-n_gu // up_steps)
        down_steps = steps - 2 - up_steps
        per_down = -(-n_dn // down_steps)

        @pl.when(s == 1)
        def _():
            finish(k)

        @pl.when(s == 2)
        def _():
            middle(k)

        up_lo = jnp.clip((s - 2) * per_up, 0, n_gu)
        gate_up(k, up_lo, jnp.where(s >= 2, jnp.clip((s - 1) * per_up, 0, n_gu), up_lo))
        at = s - 2 - up_steps
        down_lo = jnp.clip(at * per_down, 0, n_dn)
        down(k, down_lo, jnp.where(at >= 0, jnp.clip((at + 1) * per_down, 0, n_dn), down_lo))

        @pl.when(s == steps)
        def _():
            close(k)

    def ring(k):
        layer, i = divmod(k, 2)
        for b in range(2):
            for h in range(2):
                acc[i, 1, b, h, :, :] = jnp.where(lax.broadcasted_iota(jnp.int32, (hd + 8, lanes), 0) == hd, NEG, 0.0)
        if i == 0:
            for one in page_arrival(layer):
                one.wait_recv()

        def home(b, carry):
            q_t = qbuf[i, 0, b]
            s = dot32(knew[i], q_t)
            key = lax.broadcasted_iota(jnp.int32, s.shape, 0)
            tok = lax.rem(lax.broadcasted_iota(jnp.int32, s.shape, 1), part) + b * part
            s = jnp.where(key <= tok, s, NEG)
            put(acc.at[i, 0, b], *attend(layer, q_t, 2 * z + i, (s, vnew[i])))
            return carry

        lax.fori_loop(0, 2, home, 0)
        for b in range(2):
            q_hop(k, 0, b).wait_recv()
            q_hop(k, 1, b).start()

        def step(s, carry):
            def block(b, carry):
                source = lax.rem(z + jnp.where(b < 1, chips - s, s), chips)
                put(found.at[b], *attend(layer, qbuf[i, s, b], 2 * source + i, None))
                return carry

            lax.fori_loop(0, 2, block, 0)

            @pl.when(s < chips - 1)
            def _():
                for b in range(2):
                    q_hop(k, s, b).wait_recv()

                    @pl.when(s < chips - 2)
                    def _():
                        q_hop(k, s + 1, b).start()

            if k > 0:
                follow(k - 1, s)
            else:
                if layers > 1:
                    def one_page(n, carry):
                        prepare(1, n)
                        return carry

                    lax.fori_loop((s - 1) * share, jnp.minimum(s * share, pages), one_page, 0)

                @pl.when(s == chips - 1)
                def _():
                    for b in range(2):
                        q_hop(1, 0, b).start()

            @pl.when(s < chips - 1)
            def _():
                for b in range(2):
                    q_hop(k, s, b).wait_send()

            def pass_on(n, carry):
                h, b = n // 2, lax.rem(n, 2)

                @pl.when(s >= 2)
                def _():
                    a_hop(k, s - 1, b, h).wait_recv()

                @pl.when(s >= 3)
                def _():
                    a_hop(k, s - 2, b, h).wait_send()

                out, top, total = merge(take(acc.at[i, s, b, h]), take(found.at[b, h]))
                slot = lax.rem(s, 2)
                aout[i, slot, b, h, :hd, :] = out
                line = lax.broadcasted_iota(jnp.int32, (8, lanes), 0)
                aout[i, slot, b, h, hd:hd + 8, :] = jnp.where(line == 0, top, total)
                a_hop(k, s, b, h).start()
                return carry

            return lax.fori_loop(0, 4, pass_on, carry)

        lax.fori_loop(1, chips, step, 0)
        if k == 0 and layers > 1:
            prepare_end(1)

    done(load_wkv(0))
    project(0, (0, 1))
    for b in range(2):
        q_hop(0, 0, b).start()
    go(load_wo(0))
    if layers > 1:
        go(load_wkv(1))
        for pg in range(LANDS):
            page_in(1, pg).start()
    for k in range(rings):
        ring(k)
    k = rings - 1
    finish(k)
    middle(k)
    gate_up(k, 0, n_gu)
    down(k, 0, n_dn)
    close(k)
    out_ref[...] = xs[own, :]


def solution(mesh):
    group = mesh.shape["pool"]
    by_request = P(("replica", "pool"))
    by_owner = P(None, ("replica", "pool"))
    shared = P()

    def per_device(pool_loc, idx_loc, count_loc, x_loc, norm_attn, wq, wk, wv, wo, norm_mlp, w_gate, w_up, w_down):
        layers, pages, _, page, kv_heads, hd = pool_loc.shape
        slots = idx_loc.shape[2]
        tokens, d_model = x_loc.shape[1:]
        chips = group // 2
        width = wq.shape[2] // 2
        heads = width // hd
        rows = heads * tokens // 2
        ff = w_gate.shape[2] // 2
        both = 2 * tokens
        rings = 2 * layers

        meta = jnp.concatenate([idx_loc.reshape(-1), count_loc.reshape(-1)])
        meta = jnp.broadcast_to(jnp.pad(meta, (0, 128 - meta.shape[0])), (8, 128))
        raw = pool_loc.reshape(layers, pages, 2, page * kv_heads, hd)
        half = hd // 2
        freqs = ROPE_BASE ** (-jnp.arange(half, dtype=jnp.float32) / half)
        angles = jnp.arange(tokens, dtype=jnp.float32)[:, None] * freqs[None, :]
        cos_t = jnp.tile(jnp.cos(angles), (2, 2))
        sin_t = jnp.tile(jnp.concatenate([-jnp.sin(angles), jnp.sin(angles)], axis=1), (2, 1))

        def gains(one):
            return one.astype(jnp.float32)[:, None]

        vmem = pl.BlockSpec(memory_space=pltpu.VMEM)
        hbm = pl.BlockSpec(memory_space=pl.ANY)
        bf, f32 = jnp.bfloat16, jnp.float32
        dma = pltpu.SemaphoreType.DMA
        n_dn = d_model // DOWN
        out = pl.pallas_call(
            functools.partial(kernel, (group, slots)),
            out_shape=jax.ShapeDtypeStruct((tokens, d_model), bf),
            in_specs=[vmem] * 6 + [hbm] * 8,
            out_specs=vmem,
            scratch_shapes=[
                pltpu.VMEM((both, d_model), bf), pltpu.VMEM((both, d_model), bf), pltpu.VMEM((tokens, width), bf), pltpu.VMEM((both, width), bf),
                pltpu.VMEM((tokens, ff), bf),
                pltpu.VMEM((2, chips, 2, hd, rows), bf), pltpu.VMEM((2, chips + 1, 2, 2, hd + 8, rows // 2), f32),
                pltpu.VMEM((2, 2, 2, 2, hd + 8, rows // 2), f32), pltpu.VMEM((2, 2, hd + 8, rows // 2), f32),
                [pltpu.VMEM((2, pages, page, hd), bf)] * layers, [pltpu.VMEM((2, pages, hd, page), bf)] * layers,
                pltpu.VMEM((2, tokens, hd), bf), pltpu.VMEM((2, hd, tokens), bf),
                pltpu.VMEM((2 * slots, page, rows), f32),
                pltpu.VMEM((2, tokens, d_model), f32), pltpu.VMEM((2, tokens, d_model), f32),
                pltpu.VMEM((d_model, width), bf), pltpu.VMEM((2, d_model, hd), bf),
                pltpu.VMEM((PAIRS, 2, d_model, CHUNK), bf), pltpu.VMEM((DOWNS, ff, DOWN), bf),
                pltpu.VMEM((group, 8, 128), jnp.int32), pltpu.SMEM((group, 128), jnp.int32),
                pltpu.VMEM((LANDS, 2, 2 * page, hd), bf), pltpu.VMEM((2, 2 * page, hd), f32),
                pltpu.VMEM((LANDS, page, hd), bf), pltpu.VMEM((LANDS, hd, page), bf),
                dma((rings, chips, 2)), dma((rings, chips, 2)), dma((rings, chips, 2, 2)), dma((rings, chips + 1, 2, 2)),
                dma((LANDS,)), dma((LANDS, 2)), dma((layers, 2)), dma, dma,
                dma((rings, 2, n_dn)), dma((rings, 2, n_dn)),
                dma((3,)), dma((2,)), dma((PAIRS, 2)), dma((DOWNS,)),
                dma((group,)), dma((group,)), dma,
            ],
            compiler_params=pltpu.CompilerParams(collective_id=0, has_side_effects=True, vmem_limit_bytes=67000000),
        )(meta, x_loc[0], cos_t, sin_t, gains(norm_attn), gains(norm_mlp), raw, wq, wk, wv, wo, w_gate, w_up, w_down)
        return out[None]

    return jax.shard_map(per_device, mesh=mesh, in_specs=(by_owner, by_owner, by_request, by_request, shared, shared, shared, shared, shared, shared, shared, shared, shared), out_specs=by_request, check_vma=False)
```
